32 devices in a mesh: dp: 4 (over x, y), tp: 8 (over z, core).
Axes of the slice: x: 2, y: 2, z: 4, core: 2. Of those that a mesh axis runs over, the one named last changes fastest.
Arguments:
- x: bfloat16 [8192, 2048], P('dp'), parts along dimension 0
- dy: bfloat16 [8192, 2048], P('dp'), parts along dimension 0
- gate: bfloat16 [8192, 8192], P('dp', 'tp'), parts along dimension 0
- up: bfloat16 [8192, 8192], P('dp', 'tp'), parts along dimension 0
- w_gate: bfloat16 [2048, 8192], P(None, 'tp')
- w_up: bfloat16 [2048, 8192], P(None, 'tp')
- w_down: bfloat16 [8192, 2048], P('tp')
Outputs:
- output 1: bfloat16 [8192, 2048], P('dp'), parts along dimension 0
- output 2: bfloat16 [8192, 8192], P('dp', 'tp'), parts along dimension 0
- output 3: bfloat16 [8192, 8192], P('dp', 'tp'), parts along dimension 0
- output 4: bfloat16 [32768, 2048], P(('dp', 'tp')), parts along dimension 0
There are 4 independent parts. The reference program is written for one: setup_inputs(seed, part) draws one part's arguments, and reference() takes and returns one part's arrays. A program takes and returns all parts, laid end to end along the dimension named above; an argument that names none is the same for every part.
All inputs are finite; a program needn't handle non-finite values.
Results may differ from the reference program's by a relative error of at most 0.012.
Values are sent between devices in bfloat16 or wider.
A program may use at most 2 GiB of HBM per device.

```python
import jax
import jax.numpy as jnp

ROWS = 2048
D = 2048
FF = 8192


def act(gate, up):
    return jax.nn.silu(gate) * up


def setup_inputs(seed: int = 0, part: int = 0) -> dict:
    kx, ky, ka, kb, kg, ku, kd = jax.random.split(jax.random.key(seed), 7)
    kx, ky, ka, kb = (jax.random.fold_in(k, part) for k in (kx, ky, ka, kb))
    drawn = {
        "x": jax.random.normal(kx, (ROWS, D), jnp.float32),
        "dy": jax.random.normal(ky, (ROWS, D), jnp.float32),
        "gate": jax.random.normal(ka, (ROWS, FF), jnp.float32),
        "up": jax.random.normal(kb, (ROWS, FF), jnp.float32),
        "w_gate": jax.random.normal(kg, (D, FF), jnp.float32) * D**-0.5,
        "w_up": jax.random.normal(ku, (D, FF), jnp.float32) * D**-0.5,
        "w_down": jax.random.normal(kd, (FF, D), jnp.float32) * FF**-0.5,
    }
    return {k: v.astype(jnp.bfloat16) for k, v in drawn.items()}


def reference(x, dy, gate, up, w_gate, w_up, w_down):
    hidden, back = jax.vjp(act, gate.astype(jnp.float32), up.astype(jnp.float32))
    d_hidden = jnp.dot(dy, w_down.T, preferred_element_type=jnp.float32)
    d_gate, d_up = (g.astype(jnp.bfloat16) for g in back(d_hidden))
    dx = jnp.dot(d_gate, w_gate.T, preferred_element_type=jnp.float32) + jnp.dot(d_up, w_up.T, preferred_element_type=jnp.float32)
    dw_gate = jnp.dot(x.T, d_gate, preferred_element_type=jnp.float32)
    dw_up = jnp.dot(x.T, d_up, preferred_element_type=jnp.float32)
    dw_down = jnp.dot(hidden.astype(jnp.bfloat16).T, dy, preferred_element_type=jnp.float32)
    return tuple(g.astype(jnp.bfloat16) for g in (dx, dw_gate, dw_up, dw_down))
```

```python
import functools

import jax
import jax.numpy as jnp
from jax import lax
from jax.experimental import pallas as pl
from jax.experimental.pallas import tpu as pltpu
from jax.sharding import PartitionSpec as P

BF16, F32 = jnp.bfloat16, jnp.float32
MESH = pl.DeviceIdType.MESH
HALF = 1024
UNIT = 256
CHUNK = 128
NT = (((1,), (1,)), ((), ()))
NN = (((1,), (0,)), ((), ()))


def dot(a, b, dims):
    return lax.dot_general(a, b, dims, preferred_element_type=F32)


def kernel(
    x_ref, dy_ref, gate_ref, up_ref, wg_ref, wu_ref, wd_ref,
    dx_ref, dwg_ref, dwu_ref, dwd_ref,
    wd, w, dy, dg, du, hid, gu, own, stage, pt, rs, qb, ob,
    w_sem, dy_sem, gu_sem, x_sem, ob_sem, dx_sem,
    pt_send, pt_recv, rs_send, rs_recv, q_send, q_recv, dd_send, dd_recv,
):
    rows = dy_ref.shape[0]
    units, chunks = rows // UNIT, rows // CHUNK
    per = UNIT // CHUNK
    me = lax.axis_index("tp")
    z, c = me // 2, me % 2
    m = jnp.where(c == 1, z, 3 - z)
    first, last = m == 0, m == 3
    partner = z * 2 + 1 - c
    following = jnp.clip(z + 2 * c - 1, 0, 3) * 2 + c
    previous = jnp.clip(z - 2 * c + 1, 0, 3) * 2 + c
    mine = pl.multiple_of(c * HALF, HALF)
    other = pl.multiple_of((1 - c) * HALF, HALF)

    def span(i, n):
        return pl.ds(pl.multiple_of(i * n, n), n)

    def load_w(i):
        src, dst = ((wd_ref, wd), (wg_ref, w.at[0]), (wu_ref, w.at[1]))[i]
        return pltpu.make_async_copy(src, dst, w_sem.at[i])

    def load_dy(i):
        return pltpu.make_async_copy(dy_ref.at[span(i, UNIT)], dy.at[span(i, UNIT)], dy_sem.at[i])

    def load_gu(i, j):
        src = (gate_ref, up_ref)[j]
        slot = lax.rem(i, 2)
        return pltpu.make_async_copy(src.at[span(i, UNIT)], gu.at[slot, j], gu_sem.at[slot, j])

    def load_x(j):
        return pltpu.make_async_copy(x_ref.at[:, pl.ds(j * HALF, HALF)], w.at[j], x_sem.at[j])

    load_w(0).start()
    for i in range(2):
        load_dy(i).start()
        load_gu(i, 0).start()
        load_gu(i, 1).start()
        if i == 0:
            load_w(1).start()
            load_w(2).start()
    for i in range(2, units):
        load_dy(i).start()

    barrier = pltpu.get_barrier_semaphore()
    pl.semaphore_signal(barrier, inc=1, device_id={"tp": partner}, device_id_type=MESH)

    @pl.when(m < 3)
    def _():
        pl.semaphore_signal(barrier, inc=1, device_id={"tp": following}, device_id_type=MESH)

    @pl.when(m > 0)
    def _():
        pl.semaphore_signal(barrier, inc=1, device_id={"tp": previous}, device_id_type=MESH)

    pl.semaphore_wait(barrier, jnp.where(first | last, 2, 3))

    def remote(src, dst, send, recv, device):
        return pltpu.make_async_remote_copy(
            src_ref=src, dst_ref=dst, send_sem=send, recv_sem=recv,
            device_id={"tp": device}, device_id_type=MESH)

    def to_partner(k):
        r = span(k, CHUNK)
        return remote(stage.at[r], pt.at[r], pt_send.at[k], pt_recv.at[k], partner)

    def pass_sum(k):
        r = span(k, CHUNK)
        return remote(pt.at[r], rs.at[r], rs_send.at[k], rs_recv.at[k], following)

    def turn(k):
        r = span(k, CHUNK)
        return remote(pt.at[r], qb.at[r], rs_send.at[k], q_recv.at[k], partner)

    def pass_result(k):
        r = span(k, CHUNK)
        return remote(qb.at[r], qb.at[r], q_send.at[k], q_recv.at[k], following)

    def share_result(k):
        r = span(k, CHUNK)
        return remote(qb.at[r], dx_ref.at[r, pl.ds(other, HALF)], dd_send.at[k], dd_recv.at[k], partner)

    def keep_result(k):
        r = span(k, CHUNK)
        return pltpu.make_async_copy(qb.at[r], dx_ref.at[r, pl.ds(other, HALF)], dx_sem.at[0, k])

    def keep_sum(k):
        r = span(k, CHUNK)
        return pltpu.make_async_copy(pt.at[r], dx_ref.at[r, pl.ds(mine, HALF)], dx_sem.at[1, k])

    def sum_step(k, _):
        r = span(k, CHUNK)
        to_partner(k).wait_recv()

        @pl.when(first)
        def _():
            pt[r] = (own[r] + pt[r].astype(F32)).astype(BF16)

        @pl.when(m > 0)
        def _():
            pass_sum(k).wait_recv()
            pt[r] = (own[r] + pt[r].astype(F32) + rs[r].astype(F32)).astype(BF16)

        @pl.when(m < 3)
        def _():
            pass_sum(k).start()

        @pl.when(last)
        def _():
            turn(k).start()
            keep_sum(k).start()

        return 0

    def result_step(k, _):
        pass_result(k).wait_recv()

        @pl.when(m < 3)
        def _():
            pass_result(k).start()

        @pl.when(m > 0)
        def _():
            share_result(k).start()

        keep_result(k).start()
        return 0

    def paced(s):
        return jnp.maximum((s - 2 - 4 * m) * 4 + 9, 0) // 9

    def early(s):
        cap = per * ((s + 1) // 3)
        lead = jnp.where(s < 3, cap, per * (s // 3))
        return jnp.where(first, lead, jnp.minimum(paced(s), cap))

    def late(s):
        return jnp.clip(jnp.where(first, jnp.maximum(paced(s), chunks), paced(s)), 0, 2 * chunks)

    def serve(lo, hi):
        lax.fori_loop(jnp.minimum(lo, chunks), jnp.minimum(hi, chunks), sum_step, 0)
        lax.fori_loop(jnp.maximum(lo, chunks) - chunks, jnp.maximum(hi, chunks) - chunks, result_step, 0)

    def serve_sums(s):
        lax.fori_loop(early(s - 1), early(s), sum_step, 0)

    load_w(0).wait()

    def unit(u, _):
        r = span(u, UNIT)
        slot = lax.rem(u, 2)
        load_dy(u).wait()
        load_gu(u, 0).wait()
        load_gu(u, 1).wait()
        n = 512
        for b in range(0, HALF, n):
            f = slice(b, b + n)
            dh = dot(dy[r, :], wd[f, :], NT)
            gate = gu[slot, 0, :, f].astype(F32)
            up = gu[slot, 1, :, f].astype(F32)
            sig = jax.nn.sigmoid(gate)
            silu = gate * sig
            hid[r, f] = (silu * up).astype(BF16)
            du[r, f] = (dh * silu).astype(BF16)
            dg[r, f] = ((dh * up) * (sig * (1.0 + gate * (1.0 - sig)))).astype(BF16)

        @pl.when(u + 2 < units)
        def _():
            load_gu(u + 2, 0).start()
            load_gu(u + 2, 1).start()

        serve_sums(3 * u)

        @pl.when(u == 0)
        def _():
            load_w(1).wait()
            load_w(2).wait()

        stage[r] = (dot(dg[r], w[0, pl.ds(other, HALF), :], NT) + dot(du[r], w[1, pl.ds(other, HALF), :], NT)).astype(BF16)
        for j in range(per):
            to_partner(u * per + j).start()
        serve_sums(3 * u + 1)
        own[r] = dot(dg[r], w[0, pl.ds(mine, HALF), :], NT) + dot(du[r], w[1, pl.ds(mine, HALF), :], NT)
        serve_sums(3 * u + 2)
        return 0

    lax.fori_loop(0, units, unit, 0)
    for j in range(2):
        load_x(j).start()

    slots = 3 * units

    def put(i, dst):
        s = lax.rem(i, 2)
        return pltpu.make_async_copy(ob.at[s], dst, ob_sem.at[s])

    def down_dst(i):
        return dwd_ref.at[span(i // 2, UNIT), span(lax.rem(i, 2), HALF)]

    n_down = 2 * HALF // UNIT

    def down(i, _):
        @pl.when(i >= 2)
        def _():
            put(i, down_dst(0)).wait()

        left = hid[:, span(i // 2, UNIT)].T
        ob[lax.rem(i, 2)] = dot(left, dy[:, span(lax.rem(i, 2), HALF)], NN).astype(BF16)
        put(i, down_dst(i)).start()
        s = slots + i
        serve(jnp.where(i == 0, early(s - 1), late(s - 1)), late(s))
        return 0

    lax.fori_loop(0, n_down, down, 0)
    for j in range(2):
        load_x(j).wait()
    blocks = HALF // UNIT

    def side(j, right, dst):
        def body(i, _):
            put(i, dst.at[span(0, UNIT)]).wait()
            left = w[i // blocks, :, span(lax.rem(i, blocks), UNIT)].T
            ob[lax.rem(i, 2)] = dot(left, right[...], NN).astype(BF16)
            put(i, dst.at[span(i, UNIT)]).start()
            s = slots + n_down + j * 2 * blocks + i
            serve(late(s - 1), late(s))
            return 0

        lax.fori_loop(0, 2 * blocks, body, 0)

    side(0, dg, dwg_ref)
    side(1, du, dwu_ref)
    serve(late(slots + n_down + 4 * blocks - 1), 2 * chunks)

    for i in range(2):
        put(i, dwu_ref.at[span(0, UNIT)]).wait()

    def drain(k, _):
        to_partner(k).wait_send()
        keep_result(k).wait()

        @pl.when(m < 3)
        def _():
            pass_sum(k).wait_send()
            pass_result(k).wait_send()
            share_result(k).wait_recv()

        @pl.when(last)
        def _():
            turn(k).wait_send()
            keep_sum(k).wait()

        @pl.when(m > 0)
        def _():
            share_result(k).wait_send()

        return 0

    lax.fori_loop(0, chunks, drain, 0)


def backward(x, dy, gate, up, w_gate, w_up, w_down):
    rows, d = x.shape
    ff = w_down.shape[0]
    units, chunks = rows // UNIT, rows // CHUNK
    any_ = pl.BlockSpec(memory_space=pltpu.HBM)
    dma = pltpu.SemaphoreType.DMA
    half = pltpu.VMEM((rows, HALF), BF16)
    return pl.pallas_call(
        kernel,
        out_shape=[
            jax.ShapeDtypeStruct((rows, d), BF16),
            jax.ShapeDtypeStruct((d, ff), BF16),
            jax.ShapeDtypeStruct((d, ff), BF16),
            jax.ShapeDtypeStruct((ff, d), BF16),
        ],
        in_specs=[any_] * 7,
        out_specs=[any_] * 4,
        scratch_shapes=[
            pltpu.VMEM((ff, d), BF16),
            pltpu.VMEM((2, d, ff), BF16),
            pltpu.VMEM((rows, d), BF16),
            half, half, half,
            pltpu.VMEM((2, 2, UNIT, ff), BF16),
            pltpu.VMEM((rows, HALF), F32),
            half, half, half, half,
            pltpu.VMEM((2, UNIT, HALF), BF16),
            dma((3,)), dma((units,)), dma((2, 2)), dma((2,)), dma((2,)), dma((2, chunks)),
        ] + [dma((chunks,))] * 8,
        compiler_params=pltpu.CompilerParams(
            collective_id=0, has_side_effects=True, vmem_limit_bytes=67043328),
        name="mlp_backward",
    )(x, dy, gate, up, w_gate, w_up, w_down)


def solution(mesh):
    tokens, columns, rows = P("dp", None), P(None, "tp"), P("tp", None)
    return jax.shard_map(
        backward,
        mesh=mesh,
        in_specs=(tokens, tokens, P("dp", "tp"), P("dp", "tp"), columns, columns, rows),
        out_specs=(tokens, P("dp", "tp"), P("dp", "tp"), P(("dp", "tp"), None)),
        check_vma=False,
    )
```

```python
import functools

import jax
import jax.numpy as jnp
from jax import lax
from jax.experimental import pallas as pl
from jax.experimental.pallas import tpu as pltpu
from jax.sharding import PartitionSpec as P

BF16, F32 = jnp.bfloat16, jnp.float32
MESH = pl.DeviceIdType.MESH
HALF = 1024
UNIT = 256
BIG, SMALL = 128, 64
KEPT = 5
NT = (((1,), (1,)), ((), ()))
NN = (((1,), (0,)), ((), ()))


def dot(a, b, dims):
    return lax.dot_general(a, b, dims, preferred_element_type=F32)


def span(i, n):
    return pl.ds(pl.multiple_of(i * n, n), n)


def kernel(
    x_ref, dy_ref, gate_ref, up_ref, wg_ref, wu_ref, wd_ref,
    dxa, dxb, dwg, dwu, dwd,
    dy, dg, du, hid, gu, own, stage, pt, rs, xb,
    wd_sem, w_sem, dy_sem, gu_sem, x_sem, pt_send, pt_recv,
    rs_send, rs_recv, q_send, q_recv, dd_send, dd_recv,
):
    rows, d = dy.shape
    units = rows // UNIT
    per = UNIT // BIG
    n_small = UNIT // SMALL
    n_big = (units - 2) * per
    chunks = 2 * n_small + n_big
    me = lax.axis_index("tp")
    z, c = me // 2, me % 2
    m = jnp.where(c == 1, z, 3 - z)
    first, last = m == 0, m == 3
    partner = z * 2 + 1 - c
    following = jnp.clip(z + 2 * c - 1, 0, 3) * 2 + c
    previous = jnp.clip(z - 2 * c + 1, 0, 3) * 2 + c
    mine = pl.multiple_of(c * HALF, HALF)
    other = pl.multiple_of((1 - c) * HALF, HALF)

    part = HALF // 2

    def load_wd(i):
        return pltpu.make_async_copy(wd_ref.at[span(i, part)], dwd.at[span(i, part)], wd_sem.at[i])

    def load_w(i):
        src, dst = ((wg_ref, dwg), (wu_ref, dwu))[i]
        return pltpu.make_async_copy(src, dst, w_sem.at[i])

    def load_dy(i):
        return pltpu.make_async_copy(dy_ref.at[span(i, UNIT)], dy.at[span(i, UNIT)], dy_sem.at[i])

    def load_gu(i, j):
        src = (gate_ref, up_ref)[j]
        slot = lax.rem(i, 2)
        return pltpu.make_async_copy(src.at[span(i, UNIT)], gu.at[slot, j], gu_sem.at[slot, j])

    def load_x(i):
        slot = lax.rem(i, 2)
        return pltpu.make_async_copy(x_ref.at[:, span(i, UNIT)], xb.at[slot], x_sem.at[slot])

    load_dy(0).start()
    load_wd(0).start()
    load_gu(0, 0).start()
    load_gu(0, 1).start()
    load_wd(1).start()
    load_w(0).start()
    load_w(1).start()
    load_gu(1, 0).start()
    load_gu(1, 1).start()
    for i in range(1, units):
        load_dy(i).start()
    load_x(0).start()
    load_x(1).start()

    barrier = pltpu.get_barrier_semaphore()
    pl.semaphore_signal(barrier, inc=1, device_id={"tp": partner}, device_id_type=MESH)

    @pl.when(m < 3)
    def _():
        pl.semaphore_signal(barrier, inc=1, device_id={"tp": following}, device_id_type=MESH)

    @pl.when(m > 0)
    def _():
        pl.semaphore_signal(barrier, inc=1, device_id={"tp": previous}, device_id_type=MESH)

    pl.semaphore_wait(barrier, jnp.where(first | last, 2, 3))

    def remote(src, dst, send, recv, device):
        return pltpu.make_async_remote_copy(
            src_ref=src, dst_ref=dst, send_sem=send, recv_sem=recv,
            device_id={"tp": device}, device_id_type=MESH)

    def to_partner(j):
        return remote(
            stage.at[span(lax.rem(j, 2 * per), BIG)], pt.at[span(j, BIG)], pt_send.at[j], pt_recv.at[j], partner)

    def pass_sum(k, r):
        return remote(pt.at[r], rs.at[r], rs_send.at[k], rs_recv.at[k], following)

    def turn(k, r):
        return remote(dxa.at[r], dxb.at[r], rs_send.at[k], q_recv.at[k], partner)

    def pass_result(k, r):
        return remote(dxb.at[r], dxb.at[r], q_send.at[k], q_recv.at[k], following)

    def share_result(k, r):
        return remote(dxb.at[r], dxa.at[r], dd_send.at[k], dd_recv.at[k], partner)

    def sum_step(k, r, o, wait_term):
        wait_term()

        @pl.when(first)
        def _():
            pt[r] = (own[o] + pt[r].astype(F32)).astype(BF16)

        @pl.when(m > 0)
        def _():
            pass_sum(k, r).wait_recv()

        @pl.when((m > 0) & (m < 3))
        def _():
            pt[r] = (own[o] + pt[r].astype(F32) + rs[r].astype(F32)).astype(BF16)

        @pl.when(m < 3)
        def _():
            pass_sum(k, r).start()

        @pl.when(last)
        def _():
            dxa[r] = (own[o] + pt[r].astype(F32) + rs[r].astype(F32)).astype(BF16)
            turn(k, r).start()

    def result_step(k, r):
        pass_result(k, r).wait_recv()

        @pl.when(m < 3)
        def _():
            pass_result(k, r).start()

        @pl.when(m > 0)
        def _():
            share_result(k, r).start()

    def drain_step(k, r):
        @pl.when(m < 3)
        def _():
            pass_sum(k, r).wait_send()
            pass_result(k, r).wait_send()
            share_result(k, r).wait_recv()

        @pl.when(last)
        def _():
            turn(k, r).wait_send()

        @pl.when(m > 0)
        def _():
            share_result(k, r).wait_send()

    tail = n_small + n_big

    def small_row(k):
        return jnp.where(k < n_small, k, k + n_big)

    def big_row(k):
        return k - n_small + per

    def small_loop(lo, hi, step):
        def body(k, _):
            step(k, SMALL, small_row(k))
            return 0

        lax.fori_loop(lo, hi, body, 0)

    def big_loop(lo, hi, step):
        def body(k, _):
            step(k, BIG, 2 * big_row(k))
            return 0

        lax.fori_loop(lo, hi, body, 0)

    def each(lo, hi, step):
        small_loop(jnp.minimum(lo, n_small), jnp.minimum(hi, n_small), step)
        big_loop(jnp.clip(lo, n_small, tail), jnp.clip(hi, n_small, tail), step)
        small_loop(jnp.maximum(lo, tail), jnp.maximum(hi, tail), step)

    def rows_of(n, at):
        return pl.ds(pl.multiple_of(at * SMALL, n), n)

    def do_sum(k, n, at):
        kept = lax.rem(at // n_small, KEPT) * n_small + lax.rem(at, n_small)

        def wait_term():
            @pl.when(lax.rem(at, 2) == 0)
            def _():
                to_partner(at // 2).wait_recv()

        sum_step(k, rows_of(n, at), rows_of(n, kept), wait_term)

    def do_result(k, n, at):
        result_step(k, rows_of(n, at))

    def do_drain(k, n, at):
        drain_step(k, rows_of(n, at))

    blocks = rows // SMALL

    def count(n):
        n = jnp.clip(n, 0, blocks)
        return jnp.where(
            n < n_small, n,
            jnp.where(n < blocks - n_small, n_small + (n - n_small) // 2, n - (blocks - n_small) + tail))

    def paced(s):
        return jnp.maximum((s - 2) * 8 - 20 * m + 7, 0) // 7

    def early(s):
        cap = n_small * ((s + 1) // 3)
        lead = jnp.where(s < 3, cap, n_small * (s // 3))
        floor = n_small * jnp.maximum((s + 2) // 3 - KEPT, 0)
        return count(jnp.where(first, lead, jnp.minimum(jnp.maximum(paced(s), floor), cap)))

    def late(s):
        n = paced(s)
        return count(jnp.where(first, blocks, n)), count(n - blocks)

    def serve_sums(s):
        each(early(s - 1), early(s), do_sum)

    def serve(s):
        s0, r0 = late(s - 1)
        s1, r1 = late(s)
        each(s0, s1, do_sum)
        each(r0, r1, do_result)

    n = HALF // 2

    def unit(u, _):
        r = span(u, UNIT)
        slot = lax.rem(u, 2)
        load_dy(u).wait()
        for b in range(2):
            f = slice(b * n, (b + 1) * n)

            @pl.when(u == 0)
            def _():
                load_wd(b).wait()
                if b == 0:
                    load_gu(u, 0).wait()
                    load_gu(u, 1).wait()

            if b == 0:
                @pl.when(u > 0)
                def _():
                    load_gu(u, 0).wait()
                    load_gu(u, 1).wait()

            dh = dot(dy[r, :], dwd[f, :], NT)
            gate = gu[slot, 0, :, f].astype(F32)
            up = gu[slot, 1, :, f].astype(F32)
            sig = jax.nn.sigmoid(gate)
            silu = gate * sig
            hid[r, f] = (silu * up).astype(BF16)
            du[r, f] = (dh * silu).astype(BF16)
            dg[r, f] = ((dh * up) * (sig * (1.0 + gate * (1.0 - sig)))).astype(BF16)

        @pl.when(u + 2 < units)
        def _():
            load_gu(u + 2, 0).start()
            load_gu(u + 2, 1).start()

        serve_sums(3 * u)

        @pl.when(u == 0)
        def _():
            load_w(0).wait()
            load_w(1).wait()

        @pl.when(u >= 2)
        def _():
            for j in range(per):
                to_partner((u - 2) * per + j).wait_send()

        stage[span(slot, UNIT)] = (
            dot(dg[r], dwg[pl.ds(other, HALF), :], NT) + dot(du[r], dwu[pl.ds(other, HALF), :], NT)
        ).astype(BF16)
        for j in range(per):
            to_partner(u * per + j).start()
        serve_sums(3 * u + 1)
        own[span(lax.rem(u, KEPT), UNIT)] = dot(dg[r], dwg[pl.ds(mine, HALF), :], NT) + dot(du[r], dwu[pl.ds(mine, HALF), :], NT)
        serve_sums(3 * u + 2)
        return 0

    lax.fori_loop(0, units, unit, 0)

    slots = 3 * units
    each(early(slots - 1), late(slots - 1)[0], do_sum)
    halves = d // HALF
    n_down = halves * HALF // UNIT

    def down(i, _):
        left = hid[:, span(i // halves, UNIT)].T
        at = span(lax.rem(i, halves), HALF)
        dwd[span(i // halves, UNIT), at] = dot(left, dy[:, at], NN).astype(BF16)
        serve(slots + i)
        return 0

    lax.fori_loop(0, n_down, down, 0)
    n_side = d // UNIT

    def side(i, _):
        slot = lax.rem(i, 2)
        s = slots + n_down + 2 * i
        load_x(i).wait()
        left = xb[slot].T
        dwg[span(i, UNIT), :] = dot(left, dg[...], NN).astype(BF16)
        serve(s)
        left = xb[slot].T
        dwu[span(i, UNIT), :] = dot(left, du[...], NN).astype(BF16)

        @pl.when(i + 2 < n_side)
        def _():
            load_x(i + 2).start()

        serve(s + 1)
        return 0

    lax.fori_loop(0, n_side, side, 0)
    s0, r0 = late(slots + n_down + 2 * n_side - 1)
    each(s0, chunks, do_sum)
    each(r0, chunks, do_result)

    each(0, chunks, do_drain)

    def sent(j, _):
        to_partner(j).wait_send()
        return 0

    lax.fori_loop((units - 2) * per, units * per, sent, 0)


def write_out(dxa, dxb, dwg, dwu, dwd, dx_ref, dwg_ref, dwu_ref, dwd_ref, sem):
    c = lax.axis_index("tp") % 2
    mine = pl.multiple_of(c * HALF, HALF)
    other = pl.multiple_of((1 - c) * HALF, HALF)
    copies = [
        pltpu.make_async_copy(src, dst, sem.at[i])
        for i, (src, dst) in enumerate((
            (dxa, dx_ref.at[:, pl.ds(mine, HALF)]),
            (dxb, dx_ref.at[:, pl.ds(other, HALF)]),
            (dwg, dwg_ref), (dwu, dwu_ref), (dwd, dwd_ref)))
    ]
    for copy in copies:
        copy.start()
    for copy in copies:
        copy.wait()


def backward(x, dy, gate, up, w_gate, w_up, w_down):
    rows, d = x.shape
    ff = w_down.shape[0]
    units = rows // UNIT
    chunks = 2 * (UNIT // SMALL) + (units - 2) * (UNIT // BIG)
    hbm = pl.BlockSpec(memory_space=pltpu.HBM)
    vmem = pl.BlockSpec(memory_space=pltpu.VMEM)
    dma = pltpu.SemaphoreType.DMA
    half = pltpu.VMEM((rows, HALF), BF16)
    parts = pl.pallas_call(
        kernel,
        out_shape=[
            pltpu.VMEM((rows, HALF), BF16), pltpu.VMEM((rows, HALF), BF16),
            pltpu.VMEM((d, ff), BF16), pltpu.VMEM((d, ff), BF16), pltpu.VMEM((ff, d), BF16),
        ],
        in_specs=[hbm] * 7,
        out_specs=[vmem] * 5,
        scratch_shapes=[
            pltpu.VMEM((rows, d), BF16),
            half, half, half,
            pltpu.VMEM((2, 2, UNIT, ff), BF16),
            pltpu.VMEM((KEPT * UNIT, HALF), F32),
            pltpu.VMEM((2 * UNIT, HALF), BF16),
            half, half,
            pltpu.VMEM((2, rows, UNIT), BF16),
            dma((2,)), dma((2,)), dma((units,)), dma((2, 2)), dma((2,)),
            dma((rows // BIG,)), dma((rows // BIG,)),
        ] + [dma((chunks,))] * 6,
        compiler_params=pltpu.CompilerParams(
            collective_id=0, has_side_effects=True, vmem_limit_bytes=43 * 2**20),
        name="mlp_backward",
    )(x, dy, gate, up, w_gate, w_up, w_down)
    return pl.pallas_call(
        write_out,
        out_shape=[
            jax.ShapeDtypeStruct((rows, d), BF16),
            jax.ShapeDtypeStruct((d, ff), BF16),
            jax.ShapeDtypeStruct((d, ff), BF16),
            jax.ShapeDtypeStruct((ff, d), BF16),
        ],
        in_specs=[vmem] * 5,
        out_specs=[hbm] * 4,
        scratch_shapes=[dma((5,))],
        compiler_params=pltpu.CompilerParams(vmem_limit_bytes=2**20),
        name="write_out",
    )(*parts)


def solution(mesh):
    tokens, columns, rows = P("dp", None), P(None, "tp"), P("tp", None)
    return jax.shard_map(
        backward,
        mesh=mesh,
        in_specs=(tokens, tokens, P("dp", "tp"), P("dp", "tp"), columns, columns, rows),
        out_specs=(tokens, P("dp", "tp"), P("dp", "tp"), P(("dp", "tp"), None)),
        check_vma=False,
    )
```

```python
import jax
import jax.numpy as jnp
from jax import lax
from jax.experimental import pallas as pl
from jax.experimental.pallas import tpu as pltpu
from jax.sharding import PartitionSpec as P

BF16, F32 = jnp.bfloat16, jnp.float32
MESH = pl.DeviceIdType.MESH
HALF = 1024
UNIT = 256
ROWS, COLS = 128, 512
PER = 4
KEPT = 5
TICKS = (5, 7, 9, 11, 13)
NT = (((1,), (1,)), ((), ()))
NN = (((1,), (0,)), ((), ()))


def dot(a, b, dims):
    return lax.dot_general(a, b, dims, preferred_element_type=F32)


def span(i, n):
    return pl.ds(pl.multiple_of(i * n, n), n)


def kernel(
    x_ref, dy_ref, gate_ref, up_ref, wg_ref, wu_ref, wd_ref,
    dxa, dxb, dwg, dwu, dwd,
    dy, dg, du, hid, gu, own, stage, pt, rs, xb,
    wd_sem, w_sem, dy_sem, gu_sem, x_sem,
    pt_send, pt_recv, rs_send, rs_recv, q_send, q_recv, dd_send, dd_recv,
):
    rows, d = dy.shape
    units = rows // UNIT
    chunks = units * PER
    me = lax.axis_index("tp")
    z, c = me // 2, me % 2
    m = jnp.where(c == 1, z, 3 - z)
    first, last = m == 0, m == 3
    partner = z * 2 + 1 - c
    following = jnp.clip(z + 2 * c - 1, 0, 3) * 2 + c
    previous = jnp.clip(z - 2 * c + 1, 0, 3) * 2 + c
    mine, other = c * (HALF // COLS), (1 - c) * (HALF // COLS)

    def load_wd(i):
        return pltpu.make_async_copy(wd_ref.at[span(i, COLS)], dwd.at[span(i, COLS)], wd_sem.at[i])

    def load_w(i):
        at = span((other, mine)[i % 2] + i // 2, COLS)
        return [
            pltpu.make_async_copy(src.at[at], dst.at[at], w_sem.at[i, j])
            for j, (src, dst) in enumerate(((wg_ref, dwg), (wu_ref, dwu)))
        ]

    def load_dy(i):
        return pltpu.make_async_copy(dy_ref.at[span(i, UNIT)], dy.at[span(i, UNIT)], dy_sem.at[i])

    def load_gu(i):
        slot = lax.rem(i, 2)
        return [
            pltpu.make_async_copy(src.at[span(i, UNIT)], gu.at[slot, j], gu_sem.at[slot, j])
            for j, src in enumerate((gate_ref, up_ref))
        ]

    def load_x(i):
        slot = lax.rem(i, 2)
        return pltpu.make_async_copy(x_ref.at[:, span(i, UNIT)], xb.at[slot], x_sem.at[slot])

    def start(copies):
        for copy in copies:
            copy.start()

    def wait(copies):
        for copy in copies:
            copy.wait()

    start(load_gu(0))
    start([load_dy(0), load_wd(0), load_wd(1)])
    start(load_w(0) + load_w(1) + load_w(2) + load_w(3) + load_gu(1))
    start([load_dy(i) for i in range(1, units)])
    start([load_x(0), load_x(1)])

    barrier = pltpu.get_barrier_semaphore()
    pl.semaphore_signal(barrier, inc=1, device_id={"tp": partner}, device_id_type=MESH)

    @pl.when(m < 3)
    def _():
        pl.semaphore_signal(barrier, inc=1, device_id={"tp": following}, device_id_type=MESH)

    @pl.when(m > 0)
    def _():
        pl.semaphore_signal(barrier, inc=1, device_id={"tp": previous}, device_id_type=MESH)

    pl.semaphore_wait(barrier, jnp.where(first | last, 2, 3))

    def place(k, ring=0):
        u = k // PER
        if ring:
            u = lax.rem(u, ring)
        return span(u * (UNIT // ROWS) + lax.rem(k, 2), ROWS), span(lax.rem(k, PER) // 2, COLS)

    def remote(src, dst, send, recv, device):
        return pltpu.make_async_remote_copy(
            src_ref=src, dst_ref=dst, send_sem=send, recv_sem=recv,
            device_id={"tp": device}, device_id_type=MESH)

    def to_partner(k):
        return remote(stage.at[place(k, 2)], pt.at[place(k)], pt_send.at[k], pt_recv.at[k], partner)

    def pass_sum(k):
        return remote(pt.at[place(k)], rs.at[place(k)], rs_send.at[k], rs_recv.at[k], following)

    def turn(k):
        return remote(dxa.at[place(k)], dxb.at[place(k)], rs_send.at[k], q_recv.at[k], partner)

    def pass_result(k):
        return remote(dxb.at[place(k)], dxb.at[place(k)], q_send.at[k], q_recv.at[k], following)

    def share_result(k):
        return remote(dxb.at[place(k)], dxa.at[place(k)], dd_send.at[k], dd_recv.at[k], partner)

    def sum_step(k, _):
        at, kept = place(k), place(k, KEPT)
        to_partner(k).wait_recv()

        @pl.when(first)
        def _():
            pt[at] = (own[kept] + pt[at].astype(F32)).astype(BF16)

        @pl.when(m > 0)
        def _():
            pass_sum(k).wait_recv()

        @pl.when((m > 0) & (m < 3))
        def _():
            pt[at] = (own[kept] + pt[at].astype(F32) + rs[at].astype(F32)).astype(BF16)

        @pl.when(m < 3)
        def _():
            pass_sum(k).start()

        @pl.when(last)
        def _():
            dxa[at] = (own[kept] + pt[at].astype(F32) + rs[at].astype(F32)).astype(BF16)
            turn(k).start()

        return 0

    def result_step(k, _):
        pass_result(k).wait_recv()

        @pl.when(m < 3)
        def _():
            pass_result(k).start()

        @pl.when(m > 0)
        def _():
            share_result(k).start()

        return 0

    def serve(done, upto, step):
        upto = jnp.maximum(done, jnp.minimum(upto, chunks))
        lax.fori_loop(done, upto, step, 0)
        return upto

    def paced(tick):
        return jnp.maximum((tick - 8 - 10 * m) * 8 + 25, 0) // 25

    def serve_sums(done, u, sub):
        ready = PER * u + (0, 0, 2, 2, 4)[sub]
        lead = PER * u + (0, 0, 0, 2, 2)[sub]
        needed = PER * jnp.maximum(u - KEPT + (sub >= 1), 0)
        n = jnp.minimum(jnp.maximum(paced(13 * u + TICKS[sub]), needed), ready)
        return serve(done, jnp.where(first, lead, n), sum_step)

    parts = [slice(i * COLS, (i + 1) * COLS) for i in range(HALF // COLS)]

    def unit(u, done):
        r = span(u, UNIT)
        slot = lax.rem(u, 2)
        load_dy(u).wait()
        wait(load_gu(u))
        for b, f in enumerate(parts):
            @pl.when(u == 0)
            def _():
                load_wd(b).wait()

            dh = dot(dy[r, :], dwd[f, :], NT)
            gate = gu[slot, 0, :, f].astype(F32)
            up = gu[slot, 1, :, f].astype(F32)
            sig = jax.nn.sigmoid(gate)
            silu = gate * sig
            hid[r, f] = (silu * up).astype(BF16)
            du[r, f] = (dh * silu).astype(BF16)
            dg[r, f] = ((dh * up) * (sig * (1.0 + gate * (1.0 - sig)))).astype(BF16)

        @pl.when(u + 2 < units)
        def _():
            start(load_gu(u + 2))

        done = serve_sums(done, u, 0)

        @pl.when(u >= 2)
        def _():
            for j in range(PER):
                to_partner((u - 2) * PER + j).wait_send()

        for b, f in enumerate(parts):
            @pl.when(u == 0)
            def _():
                wait(load_w(2 * b))

            at = span(other + b, COLS)
            stage[span(lax.rem(u, 2), UNIT), f] = (dot(dg[r], dwg[at, :], NT) + dot(du[r], dwu[at, :], NT)).astype(BF16)
            for j in range(2):
                to_partner(u * PER + 2 * b + j).start()
            done = serve_sums(done, u, 1 + 2 * b)

            @pl.when(u == 0)
            def _():
                wait(load_w(2 * b + 1))

            at = span(mine + b, COLS)
            own[span(lax.rem(u, KEPT), UNIT), f] = dot(dg[r], dwg[at, :], NT) + dot(du[r], dwu[at, :], NT)
            done = serve_sums(done, u, 2 + 2 * b)
        return done

    done = lax.fori_loop(0, units, unit, jnp.int32(0))

    def serve_both(state, tick):
        n = paced(tick)
        sums = serve(state[0], jnp.where(first, chunks, n), sum_step)
        return sums, serve(state[1], n - chunks, result_step)

    ticks = 13 * units
    halves = d // HALF
    n_down = halves * HALF // UNIT
    n_side = d // UNIT

    def down(i, state):
        for j in range(2):
            at = span(2 * lax.rem(i, halves) + j, COLS)
            left = hid[:, span(i // halves, UNIT)].T
            dwd[span(i // halves, UNIT), at] = dot(left, dy[:, at], NN).astype(BF16)
            state = serve_both(state, ticks + 4 * i + 2 * j + 2)
        return state

    state = lax.fori_loop(0, n_down, down, (done, jnp.int32(0)))
    ticks += 4 * n_down

    def side(i, state):
        slot = lax.rem(i, 2)
        load_x(i).wait()
        for j, (right, out) in enumerate(((dg, dwg), (du, dwu))):
            for b, f in enumerate(parts):
                left = xb[slot].T
                out[span(i, UNIT), f] = dot(left, right[:, f], NN).astype(BF16)
                if j + b == 2:
                    @pl.when(i + 2 < n_side)
                    def _():
                        load_x(i + 2).start()

                state = serve_both(state, ticks + 8 * i + 4 * j + 2 * b + 2)
        return state

    state = lax.fori_loop(0, n_side, side, state)
    serve(state[0], chunks, sum_step)
    serve(state[1], chunks, result_step)

    def drain(k, _):
        @pl.when(m < 3)
        def _():
            pass_sum(k).wait_send()
            pass_result(k).wait_send()
            share_result(k).wait_recv()

        @pl.when(last)
        def _():
            turn(k).wait_send()

        @pl.when(m > 0)
        def _():
            share_result(k).wait_send()

        return 0

    lax.fori_loop(0, chunks, drain, 0)

    def sent(k, _):
        to_partner(k).wait_send()
        return 0

    lax.fori_loop((units - 2) * PER, chunks, sent, 0)


def write_out(dxa, dxb, dwg, dwu, dwd, dx_ref, dwg_ref, dwu_ref, dwd_ref, sem):
    c = lax.axis_index("tp") % 2
    copies = [
        pltpu.make_async_copy(src, dst, sem.at[i])
        for i, (src, dst) in enumerate((
            (dxa, dx_ref.at[:, span(c, HALF)]),
            (dxb, dx_ref.at[:, span(1 - c, HALF)]),
            (dwg, dwg_ref), (dwu, dwu_ref), (dwd, dwd_ref)))
    ]
    for copy in copies:
        copy.start()
    for copy in copies:
        copy.wait()


def backward(x, dy, gate, up, w_gate, w_up, w_down):
    rows, d = x.shape
    ff = w_down.shape[0]
    units = rows // UNIT
    chunks = units * PER
    hbm = pl.BlockSpec(memory_space=pltpu.HBM)
    vmem = pl.BlockSpec(memory_space=pltpu.VMEM)
    dma = pltpu.SemaphoreType.DMA
    half = pltpu.VMEM((rows, HALF), BF16)
    results = pl.pallas_call(
        kernel,
        out_shape=[
            pltpu.VMEM((rows, HALF), BF16), pltpu.VMEM((rows, HALF), BF16),
            pltpu.VMEM((d, ff), BF16), pltpu.VMEM((d, ff), BF16), pltpu.VMEM((ff, d), BF16),
        ],
        in_specs=[hbm] * 7,
        out_specs=[vmem] * 5,
        scratch_shapes=[
            pltpu.VMEM((rows, d), BF16),
            half, half, half,
            pltpu.VMEM((2, 2, UNIT, ff), BF16),
            pltpu.VMEM((KEPT * UNIT, HALF), F32),
            pltpu.VMEM((2 * UNIT, HALF), BF16),
            half, half,
            pltpu.VMEM((2, rows, UNIT), BF16),
            dma((2,)), dma((4, 2)), dma((units,)), dma((2, 2)), dma((2,)),
        ] + [dma((chunks,))] * 8,
        compiler_params=pltpu.CompilerParams(
            collective_id=0, has_side_effects=True, vmem_limit_bytes=67043328 - 20 * 2**20),
        name="mlp_backward",
    )(x, dy, gate, up, w_gate, w_up, w_down)
    return pl.pallas_call(
        write_out,
        out_shape=[
            jax.ShapeDtypeStruct((rows, d), BF16),
            jax.ShapeDtypeStruct((d, ff), BF16),
            jax.ShapeDtypeStruct((d, ff), BF16),
            jax.ShapeDtypeStruct((ff, d), BF16),
        ],
        in_specs=[vmem] * 5,
        out_specs=[hbm] * 4,
        scratch_shapes=[dma((5,))],
        compiler_params=pltpu.CompilerParams(vmem_limit_bytes=2**20),
        name="write_out",
    )(*results)


def solution(mesh):
    tokens, columns, rows = P("dp", None), P(None, "tp"), P("tp", None)
    return jax.shard_map(
        backward,
        mesh=mesh,
        in_specs=(tokens, tokens, P("dp", "tp"), P("dp", "tp"), columns, columns, rows),
        out_specs=(tokens, P("dp", "tp"), P("dp", "tp"), P(("dp", "tp"), None)),
        check_vma=False,
    )
```

```python
import jax
import jax.numpy as jnp
from jax import lax
from jax.experimental import pallas as pl
from jax.experimental.pallas import tpu as pltpu
from jax.sharding import PartitionSpec as P

BF16, F32 = jnp.bfloat16, jnp.float32
MESH = pl.DeviceIdType.MESH
HALF = 1024
UNIT = 256
ROWS, COLS = 128, 512
PER = 4
KEPT = 5
TICKS = (5, 9, 13)
NT = (((1,), (1,)), ((), ()))
NN = (((1,), (0,)), ((), ()))


def dot(a, b, dims):
    return lax.dot_general(a, b, dims, preferred_element_type=F32)


def span(i, n):
    return pl.ds(pl.multiple_of(i * n, n), n)


def kernel(
    x_ref, dy_ref, gate_ref, up_ref, wg_ref, wu_ref, wd_ref,
    dxa, dxb, dwg, dwu, dwd,
    dy, dg, du, hid, gu, own, stage, pt, rs, xb,
    wd_sem, w_sem, dy_sem, gu_sem, x_sem,
    pt_send, pt_recv, rs_send, rs_recv, q_send, q_recv, dd_send, dd_recv,
):
    rows, d = dy.shape
    units = rows // UNIT
    chunks = units * PER
    me = lax.axis_index("tp")
    z, c = me // 2, me % 2
    m = jnp.where(c == 1, z, 3 - z)
    first, last = m == 0, m == 3
    partner = z * 2 + 1 - c
    following = jnp.clip(z + 2 * c - 1, 0, 3) * 2 + c
    previous = jnp.clip(z - 2 * c + 1, 0, 3) * 2 + c
    mine, other = c, 1 - c

    def load_wd(i):
        return pltpu.make_async_copy(wd_ref.at[span(i, COLS)], dwd.at[span(i, COLS)], wd_sem.at[i])

    def load_w(i):
        at = span((other, mine)[i], HALF)
        return [
            pltpu.make_async_copy(src.at[at], dst.at[at], w_sem.at[i, j])
            for j, (src, dst) in enumerate(((wg_ref, dwg), (wu_ref, dwu)))
        ]

    def load_dy(i):
        return pltpu.make_async_copy(dy_ref.at[span(i, UNIT)], dy.at[span(i, UNIT)], dy_sem.at[i])

    def load_gu(i):
        slot = lax.rem(i, 2)
        return [
            pltpu.make_async_copy(src.at[span(i, UNIT)], gu.at[slot, j], gu_sem.at[slot, j])
            for j, src in enumerate((gate_ref, up_ref))
        ]

    def load_x(i):
        slot = lax.rem(i, 2)
        return pltpu.make_async_copy(x_ref.at[:, span(i, UNIT)], xb.at[slot], x_sem.at[slot])

    def start(copies):
        for copy in copies:
            copy.start()

    def wait(copies):
        for copy in copies:
            copy.wait()

    start(load_gu(0))
    start([load_dy(0), load_wd(0), load_wd(1)])
    start(load_w(0) + load_w(1) + load_gu(1))
    start([load_dy(i) for i in range(1, units)])
    start([load_x(0), load_x(1)])

    barrier = pltpu.get_barrier_semaphore()
    pl.semaphore_signal(barrier, inc=1, device_id={"tp": partner}, device_id_type=MESH)

    @pl.when(m < 3)
    def _():
        pl.semaphore_signal(barrier, inc=1, device_id={"tp": following}, device_id_type=MESH)

    @pl.when(m > 0)
    def _():
        pl.semaphore_signal(barrier, inc=1, device_id={"tp": previous}, device_id_type=MESH)

    pl.semaphore_wait(barrier, jnp.where(first | last, 2, 3))

    def place(k, ring=0):
        u = k // PER
        if ring:
            u = lax.rem(u, ring)
        return span(u * (UNIT // ROWS) + lax.rem(k, 2), ROWS), span(lax.rem(k, PER) // 2, COLS)

    def remote(src, dst, send, recv, device):
        return pltpu.make_async_remote_copy(
            src_ref=src, dst_ref=dst, send_sem=send, recv_sem=recv,
            device_id={"tp": device}, device_id_type=MESH)

    def to_partner(k):
        return remote(stage.at[place(k, 2)], pt.at[place(k)], pt_send.at[lax.rem(k // PER, 2)], pt_recv.at[k], partner)

    def pass_sum(k):
        return remote(pt.at[place(k)], rs.at[place(k)], rs_send, rs_recv.at[k], following)

    def turn(k):
        return remote(dxa.at[place(k)], dxb.at[place(k)], rs_send, q_recv.at[k], partner)

    def pass_result(k):
        return remote(dxb.at[place(k)], dxb.at[place(k)], q_send, q_recv.at[k], following)

    def share_result(k):
        return remote(dxb.at[place(k)], dxa.at[place(k)], dd_send, dd_recv, partner)

    def unit_sent(u):
        r = span(u, UNIT)
        return remote(
            stage.at[span(lax.rem(u, 2), UNIT)], pt.at[r], pt_send.at[lax.rem(u, 2)], pt_recv.at[0], partner)

    def sum_step(k, _):
        at, kept = place(k), place(k, KEPT)
        to_partner(k).wait_recv()

        @pl.when(first)
        def _():
            pt[at] = (own[kept] + pt[at].astype(F32)).astype(BF16)

        @pl.when(m > 0)
        def _():
            pass_sum(k).wait_recv()

        @pl.when((m > 0) & (m < 3))
        def _():
            pt[at] = (own[kept] + pt[at].astype(F32) + rs[at].astype(F32)).astype(BF16)

        @pl.when(m < 3)
        def _():
            pass_sum(k).start()

        @pl.when(last)
        def _():
            dxa[at] = (own[kept] + pt[at].astype(F32) + rs[at].astype(F32)).astype(BF16)
            turn(k).start()

        return 0

    def result_step(k, _):
        pass_result(k).wait_recv()

        @pl.when(m < 3)
        def _():
            pass_result(k).start()

        @pl.when(m > 0)
        def _():
            share_result(k).start()

        return 0

    def serve(done, upto, step):
        upto = jnp.maximum(done, jnp.minimum(upto, chunks))
        lax.fori_loop(done, upto, step, 0)
        return upto

    def paced(tick):
        return jnp.maximum((tick - 8 - 14 * m) * 9 + 25, 0) // 25

    def serve_sums(done, u, sub):
        ready = PER * (u + (sub == 2))
        needed = PER * jnp.maximum(u - KEPT + (sub >= 1), 0)
        n = jnp.minimum(jnp.maximum(paced(13 * u + TICKS[sub]), needed), ready)
        return serve(done, jnp.where(first, ready, n), sum_step)

    parts = [slice(i * COLS, (i + 1) * COLS) for i in range(HALF // COLS)]

    def unit(u, done):
        r = span(u, UNIT)
        slot = lax.rem(u, 2)
        load_dy(u).wait()
        wait(load_gu(u))
        for b, f in enumerate(parts):
            @pl.when(u == 0)
            def _():
                load_wd(b).wait()

            dh = dot(dy[r, :], dwd[f, :], NT)
            gate = gu[slot, 0, :, f].astype(F32)
            up = gu[slot, 1, :, f].astype(F32)
            sig = jax.nn.sigmoid(gate)
            silu = gate * sig
            hid[r, f] = (silu * up).astype(BF16)
            du[r, f] = (dh * silu).astype(BF16)
            dg[r, f] = ((dh * up) * (sig * (1.0 + gate * (1.0 - sig)))).astype(BF16)

        @pl.when(u + 2 < units)
        def _():
            start(load_gu(u + 2))

        done = serve_sums(done, u, 0)

        @pl.when(u >= 2)
        def _():
            unit_sent(u - 2).wait_send()

        @pl.when(u == 0)
        def _():
            wait(load_w(0))

        at = span(other, HALF)
        stage[span(lax.rem(u, 2), UNIT), :] = (dot(dg[r], dwg[at, :], NT) + dot(du[r], dwu[at, :], NT)).astype(BF16)
        for j in range(PER):
            to_partner(u * PER + j).start()
        done = serve_sums(done, u, 1)

        @pl.when(u == 0)
        def _():
            wait(load_w(1))

        at = span(mine, HALF)
        own[span(lax.rem(u, KEPT), UNIT), :] = dot(dg[r], dwg[at, :], NT) + dot(du[r], dwu[at, :], NT)
        done = serve_sums(done, u, 2)
        return done

    done = lax.fori_loop(0, units, unit, jnp.int32(0))

    def serve_both(state, tick):
        n = paced(tick)
        sums = serve(state[0], jnp.where(first, chunks, n), sum_step)
        return sums, serve(state[1], n - chunks, result_step)

    ticks = 13 * units
    halves = d // HALF
    n_down = halves * HALF // UNIT
    n_side = d // UNIT

    def down(i, state):
        at = span(lax.rem(i, halves), HALF)
        left = hid[:, span(i // halves, UNIT)].T
        dwd[span(i // halves, UNIT), at] = dot(left, dy[:, at], NN).astype(BF16)
        state = serve_both(state, ticks + 4 * i + 4)
        return state

    state = lax.fori_loop(0, n_down, down, (done, jnp.int32(0)))
    ticks += 4 * n_down

    def side(i, state):
        slot = lax.rem(i, 2)
        load_x(i).wait()
        for j, (right, out) in enumerate(((dg, dwg), (du, dwu))):
            left = xb[slot].T
            out[span(i, UNIT), :] = dot(left, right[...], NN).astype(BF16)
            if j == 1:
                @pl.when(i + 2 < n_side)
                def _():
                    load_x(i + 2).start()

            state = serve_both(state, ticks + 8 * i + 4 * j + 4)
        return state

    state = lax.fori_loop(0, n_side, side, state)
    serve(state[0], chunks, sum_step)
    serve(state[1], chunks, result_step)

    remote(dxa, dxb, rs_send, rs_recv.at[0], partner).wait_send()

    @pl.when(m < 3)
    def _():
        remote(dxb, dxb, q_send, q_recv.at[0], following).wait_send()
        remote(dxb, dxa, dd_send, dd_recv, partner).wait_recv()

    @pl.when(m > 0)
    def _():
        remote(dxb, dxa, dd_send, dd_recv, partner).wait_send()

    for u in (units - 2, units - 1):
        unit_sent(u).wait_send()


def write_out(dxa, dxb, dwg, dwu, dwd, dx_ref, dwg_ref, dwu_ref, dwd_ref, sem):
    c = lax.axis_index("tp") % 2
    copies = [
        pltpu.make_async_copy(src, dst, sem.at[i])
        for i, (src, dst) in enumerate((
            (dxa, dx_ref.at[:, span(c, HALF)]),
            (dxb, dx_ref.at[:, span(1 - c, HALF)]),
            (dwg, dwg_ref), (dwu, dwu_ref), (dwd, dwd_ref)))
    ]
    for copy in copies:
        copy.start()
    for copy in copies:
        copy.wait()


def backward(x, dy, gate, up, w_gate, w_up, w_down):
    rows, d = x.shape
    ff = w_down.shape[0]
    units = rows // UNIT
    chunks = units * PER
    hbm = pl.BlockSpec(memory_space=pltpu.HBM)
    vmem = pl.BlockSpec(memory_space=pltpu.VMEM)
    dma = pltpu.SemaphoreType.DMA
    half = pltpu.VMEM((rows, HALF), BF16)
    results = pl.pallas_call(
        kernel,
        out_shape=[
            pltpu.VMEM((rows, HALF), BF16), pltpu.VMEM((rows, HALF), BF16),
            pltpu.VMEM((d, ff), BF16), pltpu.VMEM((d, ff), BF16), pltpu.VMEM((ff, d), BF16),
        ],
        in_specs=[hbm] * 7,
        out_specs=[vmem] * 5,
        scratch_shapes=[
            pltpu.VMEM((rows, d), BF16),
            half, half, half,
            pltpu.VMEM((2, 2, UNIT, ff), BF16),
            pltpu.VMEM((KEPT * UNIT, HALF), F32),
            pltpu.VMEM((2 * UNIT, HALF), BF16),
            half, half,
            pltpu.VMEM((2, rows, UNIT), BF16),
            dma((2,)), dma((2, 2)), dma((units,)), dma((2, 2)), dma((2,)),
            dma((2,)), dma((chunks,)),
            dma, dma((chunks,)),
            dma, dma((chunks,)),
            dma, dma,
        ],
        compiler_params=pltpu.CompilerParams(
            collective_id=0, has_side_effects=True, vmem_limit_bytes=67043328 - 20 * 2**20),
        name="mlp_backward",
    )(x, dy, gate, up, w_gate, w_up, w_down)
    return pl.pallas_call(
        write_out,
        out_shape=[
            jax.ShapeDtypeStruct((rows, d), BF16),
            jax.ShapeDtypeStruct((d, ff), BF16),
            jax.ShapeDtypeStruct((d, ff), BF16),
            jax.ShapeDtypeStruct((ff, d), BF16),
        ],
        in_specs=[vmem] * 5,
        out_specs=[hbm] * 4,
        scratch_shapes=[dma((5,))],
        compiler_params=pltpu.CompilerParams(vmem_limit_bytes=2**20),
        name="write_out",
    )(*results)


def solution(mesh):
    tokens, columns, rows = P("dp", None), P(None, "tp"), P("tp", None)
    return jax.shard_map(
        backward,
        mesh=mesh,
        in_specs=(tokens, tokens, P("dp", "tp"), P("dp", "tp"), columns, columns, rows),
        out_specs=(tokens, P("dp", "tp"), P("dp", "tp"), P(("dp", "tp"), None)),
        check_vma=False,
    )
```

```python
import jax
import jax.numpy as jnp
from jax import lax
from jax.experimental import pallas as pl
from jax.experimental.pallas import tpu as pltpu
from jax.sharding import PartitionSpec as P

BF16, F32 = jnp.bfloat16, jnp.float32
MESH = pl.DeviceIdType.MESH
HALF = 1024
UNIT = 256
ROWS, COLS = 128, 512
PER = 4
KEPT = 5
TICKS = (4, 8, 12)
NT = (((1,), (1,)), ((), ()))
NN = (((1,), (0,)), ((), ()))


def dot(a, b, dims):
    return lax.dot_general(a, b, dims, preferred_element_type=F32)


def span(i, n):
    return pl.ds(pl.multiple_of(i * n, n), n)


def kernel(
    x_ref, dy_ref, gate_ref, up_ref, wg_ref, wu_ref, wd_ref,
    dxa, dxb, dwg, dwu, dwd,
    dy, dg, du, hid, gu, own, stage, pt, rs, xb,
    wd_sem, w_sem, dy_sem, gu_sem, x_sem,
    pt_send, pt_recv, rs_send, rs_recv, q_send, q_recv, dd_send, dd_recv,
):
    rows, d = dy.shape
    units = rows // UNIT
    chunks = units * PER
    me = lax.axis_index("tp")
    z, c = me // 2, me % 2
    m = jnp.where(c == 1, z, 3 - z)
    first, last = m == 0, m == 3
    partner = z * 2 + 1 - c
    following = jnp.clip(z + 2 * c - 1, 0, 3) * 2 + c
    previous = jnp.clip(z - 2 * c + 1, 0, 3) * 2 + c
    mine, other = c, 1 - c

    def load_wd(i):
        return pltpu.make_async_copy(wd_ref.at[span(i, COLS)], dwd.at[span(i, COLS)], wd_sem.at[i])

    def load_w(i):
        at = span((other, mine)[i], HALF)
        return [
            pltpu.make_async_copy(src.at[at], dst.at[at], w_sem.at[i, j])
            for j, (src, dst) in enumerate(((wg_ref, dwg), (wu_ref, dwu)))
        ]

    def load_dy(i):
        return pltpu.make_async_copy(dy_ref.at[span(i, UNIT)], dy.at[span(i, UNIT)], dy_sem.at[i])

    def load_gu(i):
        slot = lax.rem(i, 2)
        return [
            pltpu.make_async_copy(src.at[span(i, UNIT)], gu.at[slot, j], gu_sem.at[slot, j])
            for j, src in enumerate((gate_ref, up_ref))
        ]

    def load_x(i):
        slot = lax.rem(i, 2)
        return pltpu.make_async_copy(x_ref.at[:, span(i, UNIT)], xb.at[slot], x_sem.at[slot])

    def start(copies):
        for copy in copies:
            copy.start()

    def wait(copies):
        for copy in copies:
            copy.wait()

    start(load_gu(0))
    start([load_dy(0), load_wd(0), load_wd(1)])
    start(load_w(0) + load_w(1) + load_gu(1))
    start([load_dy(i) for i in range(1, units)])
    start([load_x(0), load_x(1)])

    barrier = pltpu.get_barrier_semaphore()
    pl.semaphore_signal(barrier, inc=1, device_id={"tp": partner}, device_id_type=MESH)

    @pl.when(m < 3)
    def _():
        pl.semaphore_signal(barrier, inc=1, device_id={"tp": following}, device_id_type=MESH)

    @pl.when(m > 0)
    def _():
        pl.semaphore_signal(barrier, inc=1, device_id={"tp": previous}, device_id_type=MESH)

    pl.semaphore_wait(barrier, jnp.where(first | last, 2, 3))

    def place(k, ring=0):
        u = k // PER
        if ring:
            u = lax.rem(u, ring)
        return span(u * (UNIT // ROWS) + lax.rem(k, 2), ROWS), span(lax.rem(k, PER) // 2, COLS)

    def remote(src, dst, send, recv, device):
        return pltpu.make_async_remote_copy(
            src_ref=src, dst_ref=dst, send_sem=send, recv_sem=recv,
            device_id={"tp": device}, device_id_type=MESH)

    def to_partner(k):
        return remote(stage.at[place(k, 2)], pt.at[place(k)], pt_send.at[lax.rem(k // PER, 2)], pt_recv.at[k], partner)

    def pass_sum(k):
        return remote(pt.at[place(k)], rs.at[place(k)], rs_send, rs_recv.at[k], following)

    def turn(k):
        return remote(dxa.at[place(k)], dxb.at[place(k)], rs_send, q_recv.at[k], partner)

    def pass_result(k):
        return remote(dxb.at[place(k)], dxb.at[place(k)], q_send, q_recv.at[k], following)

    def share_result(k):
        return remote(dxb.at[place(k)], dxa.at[place(k)], dd_send, dd_recv, partner)

    def unit_sent(u):
        r = span(u, UNIT)
        return remote(
            stage.at[span(lax.rem(u, 2), UNIT)], pt.at[r], pt_send.at[lax.rem(u, 2)], pt_recv.at[0], partner)

    def sum_step(k, _):
        at, kept = place(k), place(k, KEPT)
        to_partner(k).wait_recv()

        @pl.when(first)
        def _():
            pt[at] = (own[kept] + pt[at].astype(F32)).astype(BF16)

        @pl.when(m > 0)
        def _():
            pass_sum(k).wait_recv()

        @pl.when((m > 0) & (m < 3))
        def _():
            pt[at] = (own[kept] + pt[at].astype(F32) + rs[at].astype(F32)).astype(BF16)

        @pl.when(m < 3)
        def _():
            pass_sum(k).start()

        @pl.when(last)
        def _():
            dxa[at] = (own[kept] + pt[at].astype(F32) + rs[at].astype(F32)).astype(BF16)
            turn(k).start()

        return 0

    def result_step(k, _):
        pass_result(k).wait_recv()

        @pl.when(m < 3)
        def _():
            pass_result(k).start()

        @pl.when(m > 0)
        def _():
            share_result(k).start()

        return 0

    def serve(done, upto, step):
        upto = jnp.maximum(done, jnp.minimum(upto, chunks))
        lax.fori_loop(done, upto, step, 0)
        return upto

    def paced(tick):
        return jnp.maximum((tick - 8 - 14 * m) * 2 + 5, 0) // 5

    def serve_sums(done, u, sub):
        ready = PER * (u + (sub == 2))
        needed = PER * jnp.maximum(u - KEPT + (sub >= 1), 0)
        n = jnp.minimum(jnp.maximum(paced(TICKS[-1] * u + TICKS[sub]), needed), ready)
        return serve(done, jnp.where(first, ready, n), sum_step)

    parts = [slice(i * COLS, (i + 1) * COLS) for i in range(HALF // COLS)]

    def unit(u, done):
        r = span(u, UNIT)
        slot = lax.rem(u, 2)
        load_dy(u).wait()
        wait(load_gu(u))
        @pl.when(u == 0)
        def _():
            load_wd(0).wait()
            load_wd(1).wait()

        for f in [slice(i, i + 256) for i in range(0, HALF, 256)]:

            dh = dot(dy[r, :], dwd[f, :], NT)
            gate = gu[slot, 0, :, f].astype(F32)
            up = gu[slot, 1, :, f].astype(F32)
            sig = jax.nn.sigmoid(gate)
            silu = gate * sig
            hid[r, f] = (silu * up).astype(BF16)
            du[r, f] = (dh * silu).astype(BF16)
            dg[r, f] = ((dh * up) * (sig + silu * (1.0 - sig))).astype(BF16)

        @pl.when(u + 2 < units)
        def _():
            start(load_gu(u + 2))

        done = serve_sums(done, u, 0)

        @pl.when(u >= 2)
        def _():
            unit_sent(u - 2).wait_send()

        @pl.when(u == 0)
        def _():
            wait(load_w(0))

        at = span(other, HALF)
        stage[span(lax.rem(u, 2), UNIT), :] = (dot(dg[r], dwg[at, :], NT) + dot(du[r], dwu[at, :], NT)).astype(BF16)
        for j in range(PER):
            to_partner(u * PER + j).start()
        done = serve_sums(done, u, 1)

        @pl.when(u == 0)
        def _():
            wait(load_w(1))

        at = span(mine, HALF)
        own[span(lax.rem(u, KEPT), UNIT), :] = dot(dg[r], dwg[at, :], NT) + dot(du[r], dwu[at, :], NT)
        done = serve_sums(done, u, 2)
        return done

    done = lax.fori_loop(0, units, unit, jnp.int32(0))

    def serve_both(state, tick):
        n = paced(tick)
        sums = serve(state[0], jnp.where(first, chunks, n), sum_step)
        return sums, serve(state[1], n - chunks, result_step)

    ticks = TICKS[-1] * units
    halves = d // HALF
    n_down = halves * HALF // UNIT
    n_side = d // UNIT

    def down(i, state):
        at = span(lax.rem(i, halves), HALF)
        left = hid[:, span(i // halves, UNIT)].T
        dwd[span(i // halves, UNIT), at] = dot(left, dy[:, at], NN).astype(BF16)
        state = serve_both(state, ticks + 4 * i + 4)
        return state

    state = lax.fori_loop(0, n_down, down, (done, jnp.int32(0)))
    ticks += 4 * n_down

    def side(i, state):
        slot = lax.rem(i, 2)
        load_x(i).wait()
        for j, (right, out) in enumerate(((dg, dwg), (du, dwu))):
            left = xb[slot].T
            out[span(i, UNIT), :] = dot(left, right[...], NN).astype(BF16)
            if j == 1:
                @pl.when(i + 2 < n_side)
                def _():
                    load_x(i + 2).start()

            state = serve_both(state, ticks + 8 * i + 4 * j + 4)
        return state

    state = lax.fori_loop(0, n_side, side, state)
    serve(state[0], chunks, sum_step)
    serve(state[1], chunks, result_step)

    remote(dxa, dxb, rs_send, rs_recv.at[0], partner).wait_send()

    @pl.when(m < 3)
    def _():
        remote(dxb, dxb, q_send, q_recv.at[0], following).wait_send()
        remote(dxb, dxa, dd_send, dd_recv, partner).wait_recv()

    @pl.when(m > 0)
    def _():
        remote(dxb, dxa, dd_send, dd_recv, partner).wait_send()

    for u in (units - 2, units - 1):
        unit_sent(u).wait_send()


def write_out(dxa, dxb, dwg, dwu, dwd, dx_ref, dwg_ref, dwu_ref, dwd_ref, sem):
    c = lax.axis_index("tp") % 2
    copies = [
        pltpu.make_async_copy(src, dst, sem.at[i])
        for i, (src, dst) in enumerate((
            (dxa, dx_ref.at[:, span(c, HALF)]),
            (dxb, dx_ref.at[:, span(1 - c, HALF)]),
            (dwg, dwg_ref), (dwu, dwu_ref), (dwd, dwd_ref)))
    ]
    for copy in copies:
        copy.start()
    for copy in copies:
        copy.wait()


def backward(x, dy, gate, up, w_gate, w_up, w_down):
    rows, d = x.shape
    ff = w_down.shape[0]
    units = rows // UNIT
    chunks = units * PER
    hbm = pl.BlockSpec(memory_space=pltpu.HBM)
    vmem = pl.BlockSpec(memory_space=pltpu.VMEM)
    dma = pltpu.SemaphoreType.DMA
    half = pltpu.VMEM((rows, HALF), BF16)
    results = pl.pallas_call(
        kernel,
        out_shape=[
            pltpu.VMEM((rows, HALF), BF16), pltpu.VMEM((rows, HALF), BF16),
            pltpu.VMEM((d, ff), BF16), pltpu.VMEM((d, ff), BF16), pltpu.VMEM((ff, d), BF16),
        ],
        in_specs=[hbm] * 7,
        out_specs=[vmem] * 5,
        scratch_shapes=[
            pltpu.VMEM((rows, d), BF16),
            half, half, half,
            pltpu.VMEM((2, 2, UNIT, ff), BF16),
            pltpu.VMEM((KEPT * UNIT, HALF), F32),
            pltpu.VMEM((2 * UNIT, HALF), BF16),
            half, half,
            pltpu.VMEM((2, rows, UNIT), BF16),
            dma((2,)), dma((2, 2)), dma((units,)), dma((2, 2)), dma((2,)),
            dma((2,)), dma((chunks,)),
            dma, dma((chunks,)),
            dma, dma((chunks,)),
            dma, dma,
        ],
        compiler_params=pltpu.CompilerParams(
            collective_id=0, has_side_effects=True,
            vmem_limit_bytes=67043328 - 20 * 2**20),
        name="mlp_backward",
    )(x, dy, gate, up, w_gate, w_up, w_down)
    return pl.pallas_call(
        write_out,
        out_shape=[
            jax.ShapeDtypeStruct((rows, d), BF16),
            jax.ShapeDtypeStruct((d, ff), BF16),
            jax.ShapeDtypeStruct((d, ff), BF16),
            jax.ShapeDtypeStruct((ff, d), BF16),
        ],
        in_specs=[vmem] * 5,
        out_specs=[hbm] * 4,
        scratch_shapes=[dma((5,))],
        compiler_params=pltpu.CompilerParams(vmem_limit_bytes=2**20),
        name="write_out",
    )(*results)


def solution(mesh):
    tokens, columns, rows = P("dp", None), P(None, "tp"), P("tp", None)
    return jax.shard_map(
        backward,
        mesh=mesh,
        in_specs=(tokens, tokens, P("dp", "tp"), P("dp", "tp"), columns, columns, rows),
        out_specs=(tokens, P("dp", "tp"), P("dp", "tp"), P(("dp", "tp"), None)),
        check_vma=False,
    )
```

```python
import jax
import jax.numpy as jnp
from jax import lax
from jax.experimental import pallas as pl
from jax.experimental.pallas import tpu as pltpu
from jax.sharding import PartitionSpec as P

BF16, F32 = jnp.bfloat16, jnp.float32
MESH = pl.DeviceIdType.MESH
HALF = 1024
UNIT = 256
ROWS, COLS = 128, 512
PER = 4
KEPT = 5
TICKS = (4, 8, 12)
NT = (((1,), (1,)), ((), ()))
NN = (((1,), (0,)), ((), ()))


def dot(a, b, dims):
    return lax.dot_general(a, b, dims, preferred_element_type=F32)


def span(i, n):
    return pl.ds(pl.multiple_of(i * n, n), n)


def kernel(
    x_ref, dy_ref, gate_ref, up_ref, wg_ref, wu_ref, wd_ref,
    dxa, dxb, dwg, dwu, dwd,
    dy, dg, du, hid, gu, own, stage, pt, rs, xb,
    wd_sem, w_sem, dy_sem, gu_sem, x_sem,
    pt_send, pt_recv, rs_send, rs_recv, q_send, q_recv, dd_send, dd_recv,
):
    rows, d = dy.shape
    units = rows // UNIT
    chunks = units * PER
    me = lax.axis_index("tp")
    z, c = me // 2, me % 2
    m = jnp.where(c == 1, z, 3 - z)
    first, last = m == 0, m == 3
    partner = z * 2 + 1 - c
    following = jnp.clip(z + 2 * c - 1, 0, 3) * 2 + c
    previous = jnp.clip(z - 2 * c + 1, 0, 3) * 2 + c
    mine, other = c, 1 - c

    def load_wd(i):
        return pltpu.make_async_copy(wd_ref.at[span(i, COLS)], dwd.at[span(i, COLS)], wd_sem.at[i])

    def load_w(i):
        at = span((other, mine)[i], HALF)
        return [
            pltpu.make_async_copy(src.at[at], dst.at[at], w_sem.at[i, j])
            for j, (src, dst) in enumerate(((wg_ref, dwg), (wu_ref, dwu)))
        ]

    def load_dy(i):
        return pltpu.make_async_copy(dy_ref.at[span(i, UNIT)], dy.at[span(i, UNIT)], dy_sem.at[i])

    def load_gu(i):
        slot = lax.rem(i, 2)
        return [
            pltpu.make_async_copy(src.at[span(i, UNIT)], gu.at[slot, j], gu_sem.at[slot, j])
            for j, src in enumerate((gate_ref, up_ref))
        ]

    def load_x(i):
        slot = lax.rem(i, 2)
        return pltpu.make_async_copy(x_ref.at[:, span(i, UNIT)], xb.at[slot], x_sem.at[slot])

    def start(copies):
        for copy in copies:
            copy.start()

    def wait(copies):
        for copy in copies:
            copy.wait()

    start(load_gu(0))
    start([load_dy(0), load_wd(0), load_wd(1)])
    start(load_w(0) + load_w(1) + load_gu(1))
    load_dy(1).start()

    barrier = pltpu.get_barrier_semaphore()
    pl.semaphore_signal(barrier, inc=1, device_id={"tp": partner}, device_id_type=MESH)

    @pl.when(m < 3)
    def _():
        pl.semaphore_signal(barrier, inc=1, device_id={"tp": following}, device_id_type=MESH)

    @pl.when(m > 0)
    def _():
        pl.semaphore_signal(barrier, inc=1, device_id={"tp": previous}, device_id_type=MESH)

    pl.semaphore_wait(barrier, jnp.where(first | last, 2, 3))

    def place(k, ring=0):
        u = k // PER
        if ring:
            u = lax.rem(u, ring)
        return span(u * (UNIT // ROWS) + lax.rem(k, 2), ROWS), span(lax.rem(k, PER) // 2, COLS)

    def remote(src, dst, send, recv, device):
        return pltpu.make_async_remote_copy(
            src_ref=src, dst_ref=dst, send_sem=send, recv_sem=recv,
            device_id={"tp": device}, device_id_type=MESH)

    def to_partner(k):
        return remote(stage.at[place(k, 2)], pt.at[place(k)], pt_send.at[lax.rem(k // PER, 2)], pt_recv.at[k], partner)

    def pass_sum(k):
        return remote(pt.at[place(k)], rs.at[place(k)], rs_send, rs_recv.at[k], following)

    def turn(k):
        return remote(dxa.at[place(k)], dxb.at[place(k)], rs_send, q_recv.at[k], partner)

    def pass_result(k):
        return remote(dxb.at[place(k)], dxb.at[place(k)], q_send, q_recv.at[k], following)

    def share_result(k):
        return remote(dxb.at[place(k)], dxa.at[place(k)], dd_send, dd_recv, partner)

    def unit_sent(u):
        r = span(u, UNIT)
        return remote(
            stage.at[span(lax.rem(u, 2), UNIT)], pt.at[r], pt_send.at[lax.rem(u, 2)], pt_recv.at[0], partner)

    def sum_step(k, _):
        at, kept = place(k), place(k, KEPT)
        to_partner(k).wait_recv()

        @pl.when(first)
        def _():
            pt[at] = (own[kept] + pt[at].astype(F32)).astype(BF16)

        @pl.when(m > 0)
        def _():
            pass_sum(k).wait_recv()

        @pl.when((m > 0) & (m < 3))
        def _():
            pt[at] = (own[kept] + pt[at].astype(F32) + rs[at].astype(F32)).astype(BF16)

        @pl.when(m < 3)
        def _():
            pass_sum(k).start()

        @pl.when(last)
        def _():
            dxa[at] = (own[kept] + pt[at].astype(F32) + rs[at].astype(F32)).astype(BF16)
            turn(k).start()

        return 0

    def result_step(k, _):
        pass_result(k).wait_recv()

        @pl.when(m < 3)
        def _():
            pass_result(k).start()

        @pl.when(m > 0)
        def _():
            share_result(k).start()

        return 0

    def serve(done, upto, step):
        upto = jnp.maximum(done, jnp.minimum(upto, chunks))
        lax.fori_loop(done, upto, step, 0)
        return upto

    def paced(tick):
        return jnp.maximum((tick - 8 - 14 * m) * 2 + 5, 0) // 5

    def serve_sums(done, u, sub):
        ready = PER * (u + (sub == 2))
        needed = PER * jnp.maximum(u - KEPT + (sub >= 1), 0)
        n = jnp.minimum(jnp.maximum(paced(TICKS[-1] * u + TICKS[sub]), needed), ready)
        return serve(done, jnp.where(first, ready, n), sum_step)

    parts = [slice(i * COLS, (i + 1) * COLS) for i in range(HALF // COLS)]

    def unit(u, done):
        r = span(u, UNIT)
        slot = lax.rem(u, 2)
        load_dy(u).wait()
        wait(load_gu(u))
        @pl.when(u == 0)
        def _():
            load_wd(0).wait()
            load_wd(1).wait()

        for f in [slice(i, i + 256) for i in range(0, HALF, 256)]:

            dh = dot(dy[r, :], dwd[f, :], NT)
            gate = gu[slot, 0, :, f].astype(F32)
            up = gu[slot, 1, :, f].astype(F32)
            sig = jax.nn.sigmoid(gate)
            silu = gate * sig
            hid[r, f] = (silu * up).astype(BF16)
            du[r, f] = (dh * silu).astype(BF16)
            dg[r, f] = ((dh * up) * (sig + silu * (1.0 - sig))).astype(BF16)

        @pl.when(u + 2 < units)
        def _():
            start(load_gu(u + 2))
            load_dy(u + 2).start()

        @pl.when(u == units // 2)
        def _():
            start([load_x(0), load_x(1)])

        done = serve_sums(done, u, 0)

        @pl.when(u >= 2)
        def _():
            unit_sent(u - 2).wait_send()

        @pl.when(u == 0)
        def _():
            wait(load_w(0))

        at = span(other, HALF)
        stage[span(lax.rem(u, 2), UNIT), :] = (dot(dg[r], dwg[at, :], NT) + dot(du[r], dwu[at, :], NT)).astype(BF16)
        for j in range(PER):
            to_partner(u * PER + j).start()
        done = serve_sums(done, u, 1)

        @pl.when(u == 0)
        def _():
            wait(load_w(1))

        at = span(mine, HALF)
        own[span(lax.rem(u, KEPT), UNIT), :] = dot(dg[r], dwg[at, :], NT) + dot(du[r], dwu[at, :], NT)
        done = serve_sums(done, u, 2)
        return done

    done = lax.fori_loop(0, units, unit, jnp.int32(0))

    def serve_both(state, tick):
        n = paced(tick)
        sums = serve(state[0], jnp.where(first, chunks, n), sum_step)
        return sums, serve(state[1], n - chunks, result_step)

    ticks = TICKS[-1] * units
    halves = d // HALF
    n_down = halves * HALF // UNIT
    n_side = d // UNIT

    def down(i, state):
        at = span(lax.rem(i, halves), HALF)
        left = hid[:, span(i // halves, UNIT)].T
        dwd[span(i // halves, UNIT), at] = dot(left, dy[:, at], NN).astype(BF16)
        state = serve_both(state, ticks + 4 * i + 4)
        return state

    state = lax.fori_loop(0, n_down, down, (done, jnp.int32(0)))
    ticks += 4 * n_down

    def side(i, state):
        slot = lax.rem(i, 2)
        load_x(i).wait()
        for j, (right, out) in enumerate(((dg, dwg), (du, dwu))):
            left = xb[slot].T
            out[span(i, UNIT), :] = dot(left, right[...], NN).astype(BF16)
            if j == 1:
                @pl.when(i + 2 < n_side)
                def _():
                    load_x(i + 2).start()

            state = serve_both(state, ticks + 8 * i + 4 * j + 4)
        return state

    state = lax.fori_loop(0, n_side, side, state)
    serve(state[0], chunks, sum_step)
    serve(state[1], chunks, result_step)

    remote(dxa, dxb, rs_send, rs_recv.at[0], partner).wait_send()

    @pl.when(m < 3)
    def _():
        remote(dxb, dxb, q_send, q_recv.at[0], following).wait_send()
        remote(dxb, dxa, dd_send, dd_recv, partner).wait_recv()

    @pl.when(m > 0)
    def _():
        remote(dxb, dxa, dd_send, dd_recv, partner).wait_send()

    for u in (units - 2, units - 1):
        unit_sent(u).wait_send()


def write_out(dxa, dxb, dwg, dwu, dwd, dx_ref, dwg_ref, dwu_ref, dwd_ref, sem):
    c = lax.axis_index("tp") % 2
    copies = []
    for src, dst in (
        (dwg, dwg_ref), (dwu, dwu_ref), (dwd, dwd_ref),
        (dxa, dx_ref.at[:, span(c, HALF)]), (dxb, dx_ref.at[:, span(1 - c, HALF)]),
    ):
        n = src.shape[0] // 4
        for i in range(4):
            r = pl.ds(i * n, n)
            copies.append(pltpu.make_async_copy(src.at[r], dst.at[r], sem.at[len(copies)]))
    for copy in copies:
        copy.start()
    for copy in copies:
        copy.wait()


def backward(x, dy, gate, up, w_gate, w_up, w_down):
    rows, d = x.shape
    ff = w_down.shape[0]
    units = rows // UNIT
    chunks = units * PER
    hbm = pl.BlockSpec(memory_space=pltpu.HBM)
    vmem = pl.BlockSpec(memory_space=pltpu.VMEM)
    dma = pltpu.SemaphoreType.DMA
    half = pltpu.VMEM((rows, HALF), BF16)
    results = pl.pallas_call(
        kernel,
        out_shape=[
            pltpu.VMEM((rows, HALF), BF16), pltpu.VMEM((rows, HALF), BF16),
            pltpu.VMEM((d, ff), BF16), pltpu.VMEM((d, ff), BF16), pltpu.VMEM((ff, d), BF16),
        ],
        in_specs=[hbm] * 7,
        out_specs=[vmem] * 5,
        scratch_shapes=[
            pltpu.VMEM((rows, d), BF16),
            half, half, half,
            pltpu.VMEM((2, 2, UNIT, ff), BF16),
            pltpu.VMEM((KEPT * UNIT, HALF), F32),
            pltpu.VMEM((2 * UNIT, HALF), BF16),
            half, half,
            pltpu.VMEM((2, rows, UNIT), BF16),
            dma((2,)), dma((2, 2)), dma((units,)), dma((2, 2)), dma((2,)),
            dma((2,)), dma((chunks,)),
            dma, dma((chunks,)),
            dma, dma((chunks,)),
            dma, dma,
        ],
        compiler_params=pltpu.CompilerParams(
            collective_id=0, has_side_effects=True,
            vmem_limit_bytes=67043328 - 20 * 2**20),
        name="mlp_backward",
    )(x, dy, gate, up, w_gate, w_up, w_down)
    return pl.pallas_call(
        write_out,
        out_shape=[
            jax.ShapeDtypeStruct((rows, d), BF16),
            jax.ShapeDtypeStruct((d, ff), BF16),
            jax.ShapeDtypeStruct((d, ff), BF16),
            jax.ShapeDtypeStruct((ff, d), BF16),
        ],
        in_specs=[vmem] * 5,
        out_specs=[hbm] * 4,
        scratch_shapes=[dma((20,))],
        compiler_params=pltpu.CompilerParams(vmem_limit_bytes=2**20),
        name="write_out",
    )(*results)


def solution(mesh):
    tokens, columns, rows = P("dp", None), P(None, "tp"), P("tp", None)
    return jax.shard_map(
        backward,
        mesh=mesh,
        in_specs=(tokens, tokens, P("dp", "tp"), P("dp", "tp"), columns, columns, rows),
        out_specs=(tokens, P("dp", "tp"), P("dp", "tp"), P(("dp", "tp"), None)),
        check_vma=False,
    )
```

```python
import jax
import jax.numpy as jnp
from jax import lax
from jax.experimental import pallas as pl
from jax.experimental.pallas import tpu as pltpu
from jax.sharding import PartitionSpec as P

BF16, F32 = jnp.bfloat16, jnp.float32
MESH = pl.DeviceIdType.MESH
HALF = 1024
UNIT = 256
ROWS, COLS = 128, 512
PER = 4
KEPT = 5
TICKS = (4, 8, 12)
NT = (((1,), (1,)), ((), ()))
NN = (((1,), (0,)), ((), ()))


def dot(a, b, dims):
    return lax.dot_general(a, b, dims, preferred_element_type=F32)


def span(i, n):
    return pl.ds(pl.multiple_of(i * n, n), n)


def kernel(
    x_ref, dy_ref, gate_ref, up_ref, wg_ref, wu_ref, wd_ref,
    dxa, dxb, dwg, dwu, dwd,
    dy, dg, du, hid, gu, own, stage, pt, rs, xb,
    wd_sem, w_sem, dy_sem, gu_sem, x_sem,
    pt_send, pt_recv, rs_send, rs_recv, q_send, q_recv, dd_send, dd_recv,
):
    rows, d = dy.shape
    units = rows // UNIT
    chunks = units * PER
    me = lax.axis_index("tp")
    z, c = me // 2, me % 2
    m = jnp.where(c == 1, z, 3 - z)
    first, last = m == 0, m == 3
    partner = z * 2 + 1 - c
    following = jnp.clip(z + 2 * c - 1, 0, 3) * 2 + c
    previous = jnp.clip(z - 2 * c + 1, 0, 3) * 2 + c
    mine, other = c, 1 - c

    def load_wd(i):
        return pltpu.make_async_copy(wd_ref.at[span(i, COLS)], dwd.at[span(i, COLS)], wd_sem.at[i])

    def load_w(i):
        at = span((other, mine)[i], HALF)
        return [
            pltpu.make_async_copy(src.at[at], dst.at[at], w_sem.at[i, j])
            for j, (src, dst) in enumerate(((wg_ref, dwg), (wu_ref, dwu)))
        ]

    def load_dy(i):
        return pltpu.make_async_copy(dy_ref.at[span(i, UNIT)], dy.at[span(i, UNIT)], dy_sem.at[i])

    def load_gu(i):
        slot = lax.rem(i, 2)
        return [
            pltpu.make_async_copy(src.at[span(i, UNIT)], gu.at[slot, j], gu_sem.at[slot, j])
            for j, src in enumerate((gate_ref, up_ref))
        ]

    def load_x(i):
        slot = lax.rem(i, 2)
        return pltpu.make_async_copy(x_ref.at[:, span(i, UNIT)], xb.at[slot], x_sem.at[slot])

    def start(copies):
        for copy in copies:
            copy.start()

    def wait(copies):
        for copy in copies:
            copy.wait()

    start(load_gu(0))
    start([load_dy(0), load_wd(0), load_wd(1)])

    barrier = pltpu.get_barrier_semaphore()
    pl.semaphore_signal(barrier, inc=1, device_id={"tp": partner}, device_id_type=MESH)

    @pl.when(m < 3)
    def _():
        pl.semaphore_signal(barrier, inc=1, device_id={"tp": following}, device_id_type=MESH)

    @pl.when(m > 0)
    def _():
        pl.semaphore_signal(barrier, inc=1, device_id={"tp": previous}, device_id_type=MESH)

    pl.semaphore_wait(barrier, jnp.where(first | last, 2, 3))

    def place(k, ring=0):
        u = k // PER
        if ring:
            u = lax.rem(u, ring)
        return span(u * (UNIT // ROWS) + lax.rem(k, 2), ROWS), span(lax.rem(k, PER) // 2, COLS)

    def remote(src, dst, send, recv, device):
        return pltpu.make_async_remote_copy(
            src_ref=src, dst_ref=dst, send_sem=send, recv_sem=recv,
            device_id={"tp": device}, device_id_type=MESH)

    def to_partner(k):
        return remote(stage.at[place(k, 2)], pt.at[place(k)], pt_send.at[lax.rem(k // PER, 2)], pt_recv.at[k], partner)

    def pass_sum(k):
        return remote(pt.at[place(k)], rs.at[place(k)], rs_send, rs_recv.at[k], following)

    def turn(k):
        return remote(dxa.at[place(k)], dxb.at[place(k)], rs_send, q_recv.at[k], partner)

    def pass_result(k):
        return remote(dxb.at[place(k)], dxb.at[place(k)], q_send, q_recv.at[k], following)

    def share_result(k):
        return remote(dxb.at[place(k)], dxa.at[place(k)], dd_send, dd_recv, partner)

    def unit_sent(u):
        r = span(u, UNIT)
        return remote(
            stage.at[span(lax.rem(u, 2), UNIT)], pt.at[r], pt_send.at[lax.rem(u, 2)], pt_recv.at[0], partner)

    def sum_step(k, _):
        at, kept = place(k), place(k, KEPT)
        to_partner(k).wait_recv()

        @pl.when(first)
        def _():
            pt[at] = (own[kept] + pt[at].astype(F32)).astype(BF16)

        @pl.when(m > 0)
        def _():
            pass_sum(k).wait_recv()

        @pl.when((m > 0) & (m < 3))
        def _():
            pt[at] = (own[kept] + pt[at].astype(F32) + rs[at].astype(F32)).astype(BF16)

        @pl.when(m < 3)
        def _():
            pass_sum(k).start()

        @pl.when(last)
        def _():
            dxa[at] = (own[kept] + pt[at].astype(F32) + rs[at].astype(F32)).astype(BF16)
            turn(k).start()

        return 0

    def result_step(k, _):
        pass_result(k).wait_recv()

        @pl.when(m < 3)
        def _():
            pass_result(k).start()

        @pl.when(m > 0)
        def _():
            share_result(k).start()

        return 0

    def serve(done, upto, step):
        upto = jnp.maximum(done, jnp.minimum(upto, chunks))
        lax.fori_loop(done, upto, step, 0)
        return upto

    def paced(tick):
        return jnp.maximum((tick - 8 - 14 * m) * 2 + 5, 0) // 5

    def serve_sums(done, u, sub):
        ready = PER * (u + (sub == 2))
        needed = PER * jnp.maximum(u - KEPT + (sub >= 1), 0)
        n = jnp.minimum(jnp.maximum(paced(TICKS[-1] * u + TICKS[sub]), needed), ready)
        return serve(done, jnp.where(first, ready, n), sum_step)

    parts = [slice(i * COLS, (i + 1) * COLS) for i in range(HALF // COLS)]

    def unit(u, done):
        r = span(u, UNIT)
        slot = lax.rem(u, 2)
        load_dy(u).wait()
        wait(load_gu(u))
        @pl.when(u == 0)
        def _():
            start(load_w(0))
            load_wd(0).wait()
            load_wd(1).wait()
            start(load_w(1) + load_gu(1) + [load_dy(1)])

        for f in [slice(i, i + 256) for i in range(0, HALF, 256)]:

            dh = dot(dy[r, :], dwd[f, :], NT)
            gate = gu[slot, 0, :, f].astype(F32)
            up = gu[slot, 1, :, f].astype(F32)
            sig = jax.nn.sigmoid(gate)
            silu = gate * sig
            hid[r, f] = (silu * up).astype(BF16)
            du[r, f] = (dh * silu).astype(BF16)
            dg[r, f] = ((dh * up) * (sig + silu * (1.0 - sig))).astype(BF16)

        @pl.when(u + 2 < units)
        def _():
            start(load_gu(u + 2))
            load_dy(u + 2).start()

        @pl.when(u == units // 2)
        def _():
            start([load_x(0), load_x(1)])

        done = serve_sums(done, u, 0)

        @pl.when(u >= 2)
        def _():
            unit_sent(u - 2).wait_send()

        @pl.when(u == 0)
        def _():
            wait(load_w(0))

        at = span(other, HALF)
        stage[span(lax.rem(u, 2), UNIT), :] = (dot(dg[r], dwg[at, :], NT) + dot(du[r], dwu[at, :], NT)).astype(BF16)
        for j in range(PER):
            to_partner(u * PER + j).start()
        done = serve_sums(done, u, 1)

        @pl.when(u == 0)
        def _():
            wait(load_w(1))

        at = span(mine, HALF)
        own[span(lax.rem(u, KEPT), UNIT), :] = dot(dg[r], dwg[at, :], NT) + dot(du[r], dwu[at, :], NT)
        done = serve_sums(done, u, 2)
        return done

    done = lax.fori_loop(0, units, unit, jnp.int32(0))

    def serve_both(state, tick):
        n = paced(tick)
        sums = serve(state[0], jnp.where(first, chunks, n), sum_step)
        return sums, serve(state[1], n - chunks, result_step)

    ticks = TICKS[-1] * units
    halves = d // HALF
    n_down = halves * HALF // UNIT
    n_side = d // UNIT

    def down(i, state):
        at = span(lax.rem(i, halves), HALF)
        left = hid[:, span(i // halves, UNIT)].T
        dwd[span(i // halves, UNIT), at] = dot(left, dy[:, at], NN).astype(BF16)
        state = serve_both(state, ticks + 4 * i + 4)
        return state

    state = lax.fori_loop(0, n_down, down, (done, jnp.int32(0)))
    ticks += 4 * n_down

    def side(i, state):
        slot = lax.rem(i, 2)
        load_x(i).wait()
        for j, (right, out) in enumerate(((dg, dwg), (du, dwu))):
            left = xb[slot].T
            out[span(i, UNIT), :] = dot(left, right[...], NN).astype(BF16)
            if j == 1:
                @pl.when(i + 2 < n_side)
                def _():
                    load_x(i + 2).start()

            state = serve_both(state, ticks + 8 * i + 4 * j + 4)
        return state

    state = lax.fori_loop(0, n_side, side, state)
    serve(state[0], chunks, sum_step)
    serve(state[1], chunks, result_step)

    remote(dxa, dxb, rs_send, rs_recv.at[0], partner).wait_send()

    @pl.when(m < 3)
    def _():
        remote(dxb, dxb, q_send, q_recv.at[0], following).wait_send()
        remote(dxb, dxa, dd_send, dd_recv, partner).wait_recv()

    @pl.when(m > 0)
    def _():
        remote(dxb, dxa, dd_send, dd_recv, partner).wait_send()

    for u in (units - 2, units - 1):
        unit_sent(u).wait_send()


def write_out(dxa, dxb, dwg, dwu, dwd, dx_ref, dwg_ref, dwu_ref, dwd_ref, sem):
    c = lax.axis_index("tp") % 2
    copies = []
    for src, dst in (
        (dwg, dwg_ref), (dwu, dwu_ref), (dwd, dwd_ref),
        (dxa, dx_ref.at[:, span(c, HALF)]), (dxb, dx_ref.at[:, span(1 - c, HALF)]),
    ):
        n = src.shape[0] // 4
        for i in range(4):
            r = pl.ds(i * n, n)
            copies.append(pltpu.make_async_copy(src.at[r], dst.at[r], sem.at[len(copies)]))
    for copy in copies:
        copy.start()
    for copy in copies:
        copy.wait()


def backward(x, dy, gate, up, w_gate, w_up, w_down):
    rows, d = x.shape
    ff = w_down.shape[0]
    units = rows // UNIT
    chunks = units * PER
    hbm = pl.BlockSpec(memory_space=pltpu.HBM)
    vmem = pl.BlockSpec(memory_space=pltpu.VMEM)
    dma = pltpu.SemaphoreType.DMA
    half = pltpu.VMEM((rows, HALF), BF16)
    results = pl.pallas_call(
        kernel,
        out_shape=[
            pltpu.VMEM((rows, HALF), BF16), pltpu.VMEM((rows, HALF), BF16),
            pltpu.VMEM((d, ff), BF16), pltpu.VMEM((d, ff), BF16), pltpu.VMEM((ff, d), BF16),
        ],
        in_specs=[hbm] * 7,
        out_specs=[vmem] * 5,
        scratch_shapes=[
            pltpu.VMEM((rows, d), BF16),
            half, half, half,
            pltpu.VMEM((2, 2, UNIT, ff), BF16),
            pltpu.VMEM((KEPT * UNIT, HALF), F32),
            pltpu.VMEM((2 * UNIT, HALF), BF16),
            half, half,
            pltpu.VMEM((2, rows, UNIT), BF16),
            dma((2,)), dma((2, 2)), dma((units,)), dma((2, 2)), dma((2,)),
            dma((2,)), dma((chunks,)),
            dma, dma((chunks,)),
            dma, dma((chunks,)),
            dma, dma,
        ],
        compiler_params=pltpu.CompilerParams(
            collective_id=0, has_side_effects=True,
            vmem_limit_bytes=67043328 - 20 * 2**20),
        name="mlp_backward",
    )(x, dy, gate, up, w_gate, w_up, w_down)
    return pl.pallas_call(
        write_out,
        out_shape=[
            jax.ShapeDtypeStruct((rows, d), BF16),
            jax.ShapeDtypeStruct((d, ff), BF16),
            jax.ShapeDtypeStruct((d, ff), BF16),
            jax.ShapeDtypeStruct((ff, d), BF16),
        ],
        in_specs=[vmem] * 5,
        out_specs=[hbm] * 4,
        scratch_shapes=[dma((20,))],
        compiler_params=pltpu.CompilerParams(vmem_limit_bytes=2**20),
        name="write_out",
    )(*results)


def solution(mesh):
    tokens, columns, rows = P("dp", None), P(None, "tp"), P("tp", None)
    return jax.shard_map(
        backward,
        mesh=mesh,
        in_specs=(tokens, tokens, P("dp", "tp"), P("dp", "tp"), columns, columns, rows),
        out_specs=(tokens, P("dp", "tp"), P("dp", "tp"), P(("dp", "tp"), None)),
        check_vma=False,
    )
```
